32 devices in a mesh: head: 2 (over y), blk: 16 (over z, x, core).
Axes of the slice: x: 2, y: 2, z: 4, core: 2. Of those that a mesh axis runs over, the one named last changes fastest.
Arguments:
- query_rows: bfloat16 [16, 144, 3072], P('blk', 'head'), may hold values from -6 to 6
- key_rows: bfloat16 [16, 144, 3072], P('blk', 'head'), may hold values from -6 to 6
- value_rows: bfloat16 [16, 144, 3072], P('blk', 'head'), may hold values from -6 to 6
- query_tangent: bfloat16 [16, 144, 3072], P('blk', 'head'), may hold values from -6 to 6
- key_tangent: bfloat16 [16, 144, 3072], P('blk', 'head'), may hold values from -6 to 6
- value_tangent: bfloat16 [16, 144, 3072], P('blk', 'head'), may hold values from -6 to 6
- query_gain: float32 [128], replicated, may hold values from 1 to 6
- key_gain: float32 [128], replicated, may hold values from 1 to 6
Outputs:
- attended: bfloat16 [16, 144, 3072], P('blk', 'head')
- attended_tangent: bfloat16 [16, 144, 3072], P('blk', 'head')
The draws below stay inside these ranges and needn't reach their ends.
All inputs are finite; a program needn't handle non-finite values.
Results may differ from the reference program's by a relative error of at most 0.014.
The reference program's roundings to bfloat16 on the way count: a program that leaves them out, or rounds other values in their place, can miss the bound.
Values may be sent and summed in bfloat16 or wider, within the bound.
A program may use at most 64 MiB of HBM per device.

```python
import math
import jax
import jax.numpy as jnp
from jax import lax

HEADS = 24
HD = 128
D = 3072
TXT = 512
GRID_W = 64
GROUP = 16
ROWS = 144
IMAGES = 1
SEQ = 2304
BLOCKS = 16


def joint_pair(key):
    shape = (IMAGES, SEQ, D)
    key_values = jax.random.normal(jax.random.fold_in(key, 101), shape, jnp.float32)
    query_values = jax.random.normal(jax.random.fold_in(key, 102), shape, jnp.float32)

    def blocked(feature_field):
        feature_field = jnp.clip(feature_field, -6.0, 6.0).reshape(IMAGES, GROUP, ROWS, D)
        return feature_field.transpose(1, 0, 2, 3).reshape(GROUP * IMAGES, ROWS, D).astype(jnp.bfloat16)
    return (blocked(query_values), blocked(key_values))


def gain_draw(key):
    return jnp.exp(jax.random.uniform(key, (HD,), jnp.float32, 0.0, jnp.log(2.2)))


def draw_query_rows(key, part):
    return joint_pair(key)[0]


def draw_key_rows(key, part):
    return joint_pair(key)[1]


def draw_query_gain(key, part):
    return gain_draw(jax.random.fold_in(key, 201))


def draw_key_gain(key, part):
    return gain_draw(jax.random.fold_in(key, 202))


def level_of(own_key, extent, shards, least, top_value):
    factor_of = 1.0
    for dim, blocks in shards:
        heights = jax.random.uniform(jax.random.fold_in(jax.random.fold_in(own_key, 6), dim), (blocks,), jnp.float32, least / len(shards), top_value / len(shards))
        factor_of = factor_of * jnp.repeat(jnp.exp(heights), extent[dim] // blocks).reshape((-1,) + (1,) * (len(extent) - 1 - dim))
    return factor_of


def normal_values(own_key, dims, spread, bound, shards=(), held_as=jnp.bfloat16):
    loudness = level_of(own_key, dims, shards, -0.22, 0.18) if shards else 1.0
    values = jax.random.normal(own_key, dims, jnp.float32) * spread * loudness
    return jnp.minimum(jnp.maximum(values, -bound), bound).astype(held_as)


def setup_inputs(seed: int = 0) -> dict:
    key_of = jax.random.split(jax.random.key(seed), 9)
    query_rows = draw_query_rows(jax.random.fold_in(key_of[8], 71), 0)
    key_rows = draw_key_rows(jax.random.fold_in(key_of[8], 71), 0)
    value_rows = normal_values(key_of[2], (BLOCKS, ROWS, D), 1.0, 6.0, ((0, 16), (1, 2)))
    query_tangent = normal_values(key_of[3], (BLOCKS, ROWS, D), 1.0, 6.0, ((0, 16), (1, 2)))
    key_tangent = normal_values(key_of[4], (BLOCKS, ROWS, D), 1.0, 6.0, ((0, 16), (1, 2)))
    value_tangent = normal_values(key_of[5], (BLOCKS, ROWS, D), 1.0, 6.0, ((0, 16), (1, 2)))
    query_gain = draw_query_gain(jax.random.fold_in(key_of[8], 71), 0)
    key_gain = draw_key_gain(jax.random.fold_in(key_of[8], 71), 0)
    return {"query_rows": query_rows, "key_rows": key_rows, "value_rows": value_rows, "query_tangent": query_tangent, "key_tangent": key_tangent, "value_tangent": value_tangent, "query_gain": query_gain, "key_gain": key_gain}


EPSILON = 1e-06
THETA = 10000.0

def rotation(first, count, head_dim):
    block_offsets = first + jnp.arange(count, dtype=jnp.int32)
    is_image = block_offsets >= TXT
    patch = jnp.maximum(block_offsets - TXT, 0)
    row_id = jnp.where(is_image, patch // GRID_W, 0).astype(jnp.float32)
    column_id = jnp.where(is_image, patch % GRID_W, 0).astype(jnp.float32)
    leading = head_dim // 8
    lateral = (head_dim - leading) // 2
    exponent = jnp.arange(lateral // 2, dtype=jnp.float32) * (2.0 / lateral)
    frequency = jnp.exp(-math.log(THETA) * exponent)
    angles = jnp.concatenate([jnp.zeros((count, leading // 2), jnp.float32), row_id[:, None] * frequency[None, :], column_id[:, None] * frequency[None, :]], axis=1)
    angles = jnp.repeat(angles, 2, axis=1)
    return (jnp.cos(angles), jnp.sin(angles))

def rotation_partner(head_dim):
    across = jnp.arange(head_dim, dtype=jnp.int32)
    lower = across[:, None]
    upper = across[None, :]
    forward = ((upper == lower + 1) & (lower % 2 == 0)).astype(jnp.float32)
    backward = ((lower == upper + 1) & (upper % 2 == 0)).astype(jnp.float32)
    return forward - backward

def normalize(raw, tangent, gain, cosine, sine, partner):
    values = raw.astype(jnp.float32)
    motion = tangent.astype(jnp.float32)
    inverse = lax.rsqrt(lax.optimization_barrier(jnp.mean(values * values, axis=-1, keepdims=True)) + EPSILON)
    coupling = lax.optimization_barrier(jnp.mean(values * motion, axis=-1, keepdims=True))
    normed = values * inverse * gain
    normalized_tangent = gain * (motion * inverse - values * inverse * inverse * inverse * coupling)

    def rotate(feature_field):
        return feature_field * cosine + jnp.dot(feature_field, partner, precision=lax.Precision.HIGHEST) * sine
    return (rotate(normed).astype(jnp.bfloat16), rotate(normalized_tangent).astype(jnp.bfloat16))

def attend(item):
    query_hat, query_dot, key_hat, key_dot, value, value_dot = [feature_field.astype(jnp.float32) for feature_field in item]
    scale = 1.0 / math.sqrt(HD)
    logit_scores = jnp.dot(query_hat, key_hat.T, preferred_element_type=jnp.float32) * scale
    peak = lax.optimization_barrier(jnp.max(logit_scores, axis=1, keepdims=True))
    weights = jnp.exp(logit_scores - peak)
    total = lax.optimization_barrier(jnp.sum(weights, axis=1, keepdims=True))
    score_dot = (jnp.dot(query_dot, key_hat.T, preferred_element_type=jnp.float32) + jnp.dot(query_hat, key_dot.T, preferred_element_type=jnp.float32)) * scale
    product = weights * score_dot
    drift = lax.optimization_barrier(jnp.sum(product, axis=1, keepdims=True))
    low_weights = lax.optimization_barrier(weights.astype(jnp.bfloat16)).astype(jnp.float32)
    low_product = lax.optimization_barrier(product.astype(jnp.bfloat16)).astype(jnp.float32)
    summed = jnp.dot(low_weights, value, preferred_element_type=jnp.float32)
    summed_dot = jnp.dot(low_weights, value_dot, preferred_element_type=jnp.float32) + jnp.dot(low_product, value, preferred_element_type=jnp.float32)
    attention_output = (summed / total).astype(jnp.bfloat16)
    output_tangent = ((summed_dot - drift / total * summed) / total).astype(jnp.bfloat16)
    return (attention_output, output_tangent)

def reference(query_rows, key_rows, value_rows, query_tangent, key_tangent, value_tangent, query_gain, key_gain):

    def unblock(blocked):
        return blocked.reshape(GROUP, IMAGES, ROWS, HEADS, HD).transpose(1, 0, 2, 3, 4).reshape(IMAGES, SEQ, HEADS, HD)
    cosine, sine = rotation(0, SEQ, HD)
    cosine = cosine[None, :, None, :]
    sine = sine[None, :, None, :]
    partner = rotation_partner(HD)
    query_hat, query_dot = normalize(unblock(query_rows), unblock(query_tangent), query_gain, cosine, sine, partner)
    key_hat, key_dot = normalize(unblock(key_rows), unblock(key_tangent), key_gain, cosine, sine, partner)

    def per_head_split(feature_field):
        return feature_field.transpose(0, 2, 1, 3).reshape(IMAGES * HEADS, SEQ, HD)
    items = tuple((per_head_split(feature_field) for feature_field in (query_hat, query_dot, key_hat, key_dot, unblock(value_rows), unblock(value_tangent))))
    attention_output, output_tangent = lax.map(attend, items)

    def regroup_blocks(feature_field):
        feature_field = feature_field.reshape(IMAGES, HEADS, SEQ, HD).transpose(0, 2, 1, 3)
        feature_field = feature_field.reshape(IMAGES, GROUP, ROWS, HEADS * HD).transpose(1, 0, 2, 3)
        return feature_field.reshape(GROUP * IMAGES, ROWS, HEADS * HD)
    return (regroup_blocks(attention_output), regroup_blocks(output_tangent))
```

```python
import functools
import math

import jax
import jax.numpy as jnp
from jax import lax
from jax.experimental import pallas as pl
from jax.experimental.pallas import tpu as pltpu
from jax.sharding import PartitionSpec as P

HD = 128
TXT = 512
GRID_W = 64
GROUP = 16


EPSILON = 1e-06
THETA = 10000.0


def passed_along(block, axis, distance):
    devices = range(lax.axis_size(axis))
    route = [((i - distance) % len(devices), i) for i in devices]
    return lax.ppermute(block, axis, route)


def rotation(first, count, head_dim):
    block_offsets = first + jnp.arange(count, dtype=jnp.int32)
    is_image = block_offsets >= TXT
    patch = jnp.maximum(block_offsets - TXT, 0)
    row_id = jnp.where(is_image, patch // GRID_W, 0).astype(jnp.float32)
    column_id = jnp.where(is_image, patch % GRID_W, 0).astype(jnp.float32)
    leading = head_dim // 8
    lateral = (head_dim - leading) // 2
    exponent = jnp.arange(lateral // 2, dtype=jnp.float32) * (2.0 / lateral)
    frequency = jnp.exp(-math.log(THETA) * exponent)
    angles = jnp.concatenate(
        [
            jnp.zeros((count, leading // 2), jnp.float32),
            row_id[:, None] * frequency[None, :],
            column_id[:, None] * frequency[None, :],
        ],
        axis=1,
    )
    angles = jnp.repeat(angles, 2, axis=1)
    return (jnp.cos(angles), jnp.sin(angles))


def rotation_partner(head_dim):
    across = jnp.arange(head_dim, dtype=jnp.int32)
    lower = across[:, None]
    upper = across[None, :]
    forward = ((upper == lower + 1) & (lower % 2 == 0)).astype(jnp.float32)
    backward = ((lower == upper + 1) & (upper % 2 == 0)).astype(jnp.float32)
    return forward - backward


def normalize(raw, tangent, gain, cosine, sine, partner):
    values = raw.astype(jnp.float32)
    motion = tangent.astype(jnp.float32)
    inverse = lax.rsqrt(jnp.mean(values * values, axis=-1, keepdims=True) + EPSILON)
    coupling = jnp.mean(values * motion, axis=-1, keepdims=True)
    normed = values * inverse * gain
    normalized_tangent = gain * (motion * inverse - values * inverse * inverse * inverse * coupling)

    def rotate(feature_field):
        return (
            feature_field * cosine
            + jnp.dot(feature_field, partner, precision=lax.Precision.HIGHEST) * sine
        )

    return (rotate(normed).astype(jnp.bfloat16), rotate(normalized_tangent).astype(jnp.bfloat16))


def local(
    query_rows,
    key_rows,
    value_rows,
    query_tangent,
    key_tangent,
    value_tangent,
    query_gain,
    key_gain,
):
    arrived = (
        lax.all_to_all(query_rows, "head", split_axis=2, concat_axis=1, tiled=True),
        lax.all_to_all(key_rows, "head", split_axis=2, concat_axis=1, tiled=True),
        lax.all_to_all(value_rows, "head", split_axis=2, concat_axis=1, tiled=True),
        lax.all_to_all(query_tangent, "head", split_axis=2, concat_axis=1, tiled=True),
        lax.all_to_all(key_tangent, "head", split_axis=2, concat_axis=1, tiled=True),
        lax.all_to_all(value_tangent, "head", split_axis=2, concat_axis=1, tiled=True),
    )
    rows_here = arrived[0].shape[1]
    local_width = arrived[0].shape[2]
    heads_here = local_width // HD
    images = lax.axis_size("blk") // GROUP
    place = lax.axis_index("blk") // images

    def split_heads(feature_field):
        return feature_field[0].reshape(rows_here, heads_here, HD)

    cosine, sine = rotation(place * rows_here, rows_here, HD)
    cosine = cosine[:, None, :]
    sine = sine[:, None, :]
    partner = rotation_partner(HD)
    query_hat, query_dot = normalize(
        split_heads(arrived[0]), split_heads(arrived[3]), query_gain, cosine, sine, partner
    )
    key_hat, key_dot = normalize(
        split_heads(arrived[1]), split_heads(arrived[4]), key_gain, cosine, sine, partner
    )
    own_block = jnp.stack(
        [
            key_hat.reshape(rows_here, local_width),
            arrived[2][0],
            key_dot.reshape(rows_here, local_width),
            arrived[5][0],
        ],
        axis=0,
    )
    scale = 1.0 / math.sqrt(HD)
    query_pair = jnp.concatenate([query_dot, query_hat], axis=2)

    def absorb_segment(state, key_block):
        peak, total, drift, summed, summed_dot = state
        count = key_block.shape[1]
        block_key = key_block[0].reshape(count, heads_here, HD)
        block_value = key_block[1].reshape(count, heads_here, HD)
        block_key_dot = key_block[2].reshape(count, heads_here, HD)
        block_value_dot = key_block[3].reshape(count, heads_here, HD)
        logit_scores = (
            jnp.einsum("qhd,khd->hqk", query_hat, block_key, preferred_element_type=jnp.float32)
            * scale
        )
        key_pair = jnp.concatenate([block_key, block_key_dot], axis=2)
        score_dot = (
            jnp.einsum("qhd,khd->hqk", query_pair, key_pair, preferred_element_type=jnp.float32)
            * scale
        )
        new_peak = jnp.maximum(peak, jnp.max(logit_scores, axis=2, keepdims=True))
        rescale = jnp.exp(peak - new_peak)
        weights = jnp.exp(logit_scores - new_peak)
        product = weights * score_dot
        total = total * rescale + jnp.sum(weights, axis=2, keepdims=True)
        drift = drift * rescale + jnp.sum(product, axis=2, keepdims=True)
        low_weights = weights.astype(jnp.bfloat16)
        low_product = product.astype(jnp.bfloat16)
        summed = summed * rescale + jnp.einsum(
            "hqk,khd->hqd", low_weights, block_value, preferred_element_type=jnp.float32
        )
        summed_dot = (
            summed_dot * rescale
            + jnp.einsum(
                "hqk,khd->hqd", low_weights, block_value_dot, preferred_element_type=jnp.float32
            )
            + jnp.einsum(
                "hqk,khd->hqd", low_product, block_value, preferred_element_type=jnp.float32
            )
        )
        return (new_peak, total, drift, summed, summed_dot)

    def absorb(state, key_block):
        count = key_block.shape[1]
        span = 2 * rows_here
        return absorb_segment(state, key_block)

    state = (
        jnp.full((heads_here, rows_here, 1), -jnp.inf, jnp.float32),
        jnp.zeros((heads_here, rows_here, 1), jnp.float32),
        jnp.zeros((heads_here, rows_here, 1), jnp.float32),
        jnp.zeros((heads_here, rows_here, HD), jnp.float32),
        jnp.zeros((heads_here, rows_here, HD), jnp.float32),
    )

    def pass_on(key_block):
        return passed_along(key_block, "blk", images)

    def pair_step(counter, carry):
        carried, current = carry
        following = pass_on(current)
        carried = absorb(carried, jnp.concatenate([current, following], axis=1))
        current = pass_on(following)
        return (carried, current)

    state, current = lax.fori_loop(0, GROUP // 2 - 1, pair_step, (state, own_block))
    following = pass_on(current)
    state = absorb(state, jnp.concatenate([current, following], axis=1))
    peak, total, drift, summed, summed_dot = state
    attention_output = summed / total
    output_tangent = (summed_dot - drift / total * summed) / total
    attention_output = (
        attention_output.transpose(1, 0, 2)
        .reshape(rows_here, local_width)
        .astype(jnp.bfloat16)[None]
    )
    output_tangent = (
        output_tangent.transpose(1, 0, 2).reshape(rows_here, local_width).astype(jnp.bfloat16)[None]
    )
    returned = (
        lax.all_to_all(attention_output, "head", split_axis=1, concat_axis=2, tiled=True),
        lax.all_to_all(output_tangent, "head", split_axis=1, concat_axis=2, tiled=True),
    )
    return (returned[0], returned[1])


MESH = pl.DeviceIdType.MESH
ARRAYS = 4


def prepare_kernel(q, k, v, qt, kt, vt, qg, kg, cos_ref, before_ref, after_ref, kv_out, q_out):
    cosine, before, after = cos_ref[...], before_ref[...], after_ref[...]

    def rotate(x):
        return x * cosine + pltpu.roll(x, HD - 1, 1) * before + pltpu.roll(x, 1, 1) * after

    def pair(raw, tangent, gain):
        values = raw.astype(jnp.float32)
        motion = tangent.astype(jnp.float32)
        inverse = lax.rsqrt(jnp.mean(values * values, axis=-1, keepdims=True) + EPSILON)
        coupling = jnp.mean(values * motion, axis=-1, keepdims=True)
        normed = values * inverse * gain
        moved = gain * (motion * inverse - values * (inverse * inverse * inverse * coupling))
        return rotate(normed).astype(jnp.bfloat16), rotate(moved).astype(jnp.bfloat16)

    for head in range(q.shape[1] // HD):
        columns = slice(head * HD, (head + 1) * HD)
        q_hat, q_dot = pair(q[:, columns], qt[:, columns], qg[...])
        k_hat, k_dot = pair(k[:, columns], kt[:, columns], kg[...])
        q_out[head, 0] = q_hat
        q_out[head, 1] = q_dot
        kv_out[head, 0] = k_hat
        kv_out[head, 1] = k_dot
        kv_out[head, 2] = v[:, columns]
        kv_out[head, 3] = vt[:, columns]


def prepare(arrays, gains, tables, heads_each):
    rows, width = arrays[0].shape
    heads = width // HD
    block = pl.BlockSpec((rows, heads_each * HD), lambda i: (0, i))
    gain = pl.BlockSpec((1, HD), lambda i: (0, 0))
    table = pl.BlockSpec((rows, HD), lambda i: (0, 0))
    return pl.pallas_call(
        prepare_kernel,
        grid=(heads // heads_each,),
        in_specs=[block] * 6 + [gain] * 2 + [table] * 3,
        out_specs=[
            pl.BlockSpec((heads_each, ARRAYS, rows, HD), lambda i: (i, 0, 0, 0)),
            pl.BlockSpec((heads_each, 2, rows, HD), lambda i: (i, 0, 0, 0)),
        ],
        out_shape=[
            jax.ShapeDtypeStruct((heads, ARRAYS, rows, HD), jnp.bfloat16),
            jax.ShapeDtypeStruct((heads, 2, rows, HD), jnp.bfloat16),
        ],
        compiler_params=pltpu.CompilerParams(dimension_semantics=("arbitrary",)),
    )(*arrays, *gains, *tables)


def joint_kernel(
    n_head, ring, heads_each, rows,
    kv_ref, q_ref, out_ref,
    kv_held, q_held, sent, peak_s, total_s, drift_s, sum_s, dot_s,
    kv_send, kv_recv, pass_send, pass_recv, q_send, q_recv, o_send, o_recv,
):
    chips = n_head * ring
    y = lax.axis_index("head")
    n = lax.axis_index("blk")
    core = n % 2
    half = n // (2 * ring)
    r = (n // 2) % ring
    group = y * ring + r

    def chip(offset, far):
        return (y + offset // ring) % n_head, (r + offset % ring) % ring, (half + far) % 2

    def device(offset, far):
        ty, tr, th = chip(offset, far)
        return (ty, (th * ring + tr) * 2 + core)

    def source(offset):
        ty = (y + n_head - offset // ring) % n_head
        tr = (r + ring - offset % ring) % ring
        return ty, tr, (ty, (half * ring + tr) * 2 + core)

    partner = (y, (half * ring + r) * 2 + 1 - core)

    barrier = pltpu.get_barrier_semaphore()
    for far in range(2):
        for offset in range(chips):
            if far or offset:
                pl.semaphore_signal(barrier, inc=1, device_id=device(offset, far), device_id_type=MESH)
    pl.semaphore_signal(barrier, inc=1, device_id=partner, device_id_type=MESH)
    pl.semaphore_wait(barrier, 2 * chips)

    def kv_copy(j, offset, far):
        ty, tr, _ = chip(offset, far)
        return pltpu.make_async_remote_copy(
            src_ref=kv_ref.at[(ty * ring + tr) * heads_each + j],
            dst_ref=kv_held.at[far, j, :, pl.ds(pl.multiple_of(offset * 2 * rows, 8), rows), :],
            send_sem=kv_send.at[far, j, offset],
            recv_sem=kv_recv.at[far, j, offset],
            device_id=device(offset, far),
            device_id_type=MESH,
        )

    def pass_copy(j, offset, far):
        slot = kv_held.at[far, j, :, pl.ds(pl.multiple_of(offset * 2 * rows, 8), rows), :]
        own = isinstance(offset, int) and offset == 0 and far == 0
        return pltpu.make_async_remote_copy(
            src_ref=kv_ref.at[group * heads_each + j] if own else slot,
            dst_ref=kv_held.at[far, j, :, pl.ds(pl.multiple_of((offset * 2 + 1) * rows, 8), rows), :],
            send_sem=pass_send.at[far, j, offset],
            recv_sem=pass_recv.at[far, j, offset],
            device_id=partner,
            device_id_type=MESH,
        )

    def q_copy(offset):
        ty, tr, _ = chip(offset, 0)
        return pltpu.make_async_remote_copy(
            src_ref=q_ref.at[pl.ds((ty * ring + tr) * heads_each, heads_each)],
            dst_ref=q_held.at[:, :, pl.ds(pl.multiple_of(offset * rows, 8), rows), :],
            send_sem=q_send.at[offset],
            recv_sem=q_recv.at[offset],
            device_id=device(offset, 0),
            device_id_type=MESH,
        )

    def o_copy(j, offset):
        _, _, there = source(offset)
        return pltpu.make_async_remote_copy(
            src_ref=sent.at[j, :, pl.ds(pl.multiple_of(offset * rows, 8), rows), :],
            dst_ref=out_ref.at[group * heads_each + j],
            send_sem=o_send.at[j, offset],
            recv_sem=o_recv.at[j, offset],
            device_id=there,
            device_id_type=MESH,
        )

    def each(low, body):
        @pl.loop(low, chips)
        def _(offset):
            body(offset)

    def start_kv(j, far):
        each(1 - far, lambda offset: kv_copy(j, offset, far).start())

    start_kv(0, 1)
    each(1, lambda offset: q_copy(offset).start())
    start_kv(0, 0)
    for j in range(heads_each):
        pass_copy(j, 0, 0).start()
    for j in range(1, heads_each):
        start_kv(j, 1)
        start_kv(j, 0)
    mine = pl.ds(group * heads_each, heads_each)
    q_held[:, :, 0:rows, :] = q_ref[mine]
    kv_held[0, :, :, 0:rows, :] = kv_ref[mine]

    scale = 1.0 / math.sqrt(HD)
    keys = 2 * chips * rows
    tile = 2 * rows

    def arrive(j, far):
        def step(offset):
            kv_copy(j, offset, far).wait_recv()
            pass_copy(j, offset, far).start()

        each(1 - far, step)

    def attend(j, far):
        if far == 0:
            pass_copy(j, 0, 0).wait_recv()
        each(1 - far, lambda offset: pass_copy(j, offset, far).wait_recv())

        @pl.loop(0, chips * rows // tile)
        def _(t):
            at = pl.ds(pl.multiple_of(t * tile, tile), tile)
            q_hat = q_held[j, 0, at, :]
            q_dot = q_held[j, 1, at, :]
            k_hat, k_dot = kv_held[far, j, 0], kv_held[far, j, 1]
            v, v_dot = kv_held[far, j, 2], kv_held[far, j, 3]
            dims = (((1,), (1,)), ((), ()))
            scores = lax.dot_general(q_hat, k_hat, dims, preferred_element_type=jnp.float32) * scale
            moved = lax.dot_general(
                jnp.concatenate([q_dot, q_hat], axis=1),
                jnp.concatenate([k_hat, k_dot], axis=1),
                dims,
                preferred_element_type=jnp.float32,
            ) * scale
            peak = jnp.max(scores, axis=1, keepdims=True)
            if far:
                old = peak_s[at, :1]
                peak = jnp.maximum(peak, old)
            weights = jnp.exp(scores - peak)
            product = weights * moved
            total = jnp.sum(weights, axis=1, keepdims=True)
            drift = jnp.sum(product, axis=1, keepdims=True)
            low = weights.astype(jnp.bfloat16)
            both = jnp.dot(low, jnp.concatenate([v, v_dot], axis=1), preferred_element_type=jnp.float32)
            summed = both[:, :HD]
            summed_dot = both[:, HD:] + jnp.dot(
                product.astype(jnp.bfloat16), v, preferred_element_type=jnp.float32
            )
            if far:
                again = jnp.exp(old - peak)
                total = total + again * total_s[at, :1]
                drift = drift + again * drift_s[at, :1]
                summed = summed + again * sum_s[at, :]
                summed_dot = summed_dot + again * dot_s[at, :]
                sent[j, 0, at, :] = (summed / total).astype(jnp.bfloat16)
                sent[j, 1, at, :] = ((summed_dot - (drift / total) * summed) / total).astype(jnp.bfloat16)
            else:
                peak_s[at, :] = jnp.broadcast_to(peak, (tile, HD))
                total_s[at, :] = jnp.broadcast_to(total, (tile, HD))
                drift_s[at, :] = jnp.broadcast_to(drift, (tile, HD))
                sum_s[at, :] = summed
                dot_s[at, :] = summed_dot

    each(1, lambda offset: q_copy(offset).wait_recv())
    stages = [(j, far) for j in range(heads_each) for far in range(2)]
    arrive(*stages[0])
    for index, (j, far) in enumerate(stages):
        if index + 1 < len(stages) and far == 0:
            attend(j, far)
            arrive(*stages[index + 1])
        elif index + 1 < len(stages):
            arrive(*stages[index + 1])
            attend(j, far)
        else:
            attend(j, far)
        if far:
            each(1, lambda offset: o_copy(j, offset).start())
            out_ref[group * heads_each + j] = sent[j, :, 0:rows, :]

    for j in range(heads_each):
        for far in range(2):
            each(1 - far, lambda offset: kv_copy(j, offset, far).wait_send())
            if far == 0:
                pass_copy(j, 0, 0).wait_send()
            each(1 - far, lambda offset: pass_copy(j, offset, far).wait_send())
    each(1, lambda offset: q_copy(offset).wait_send())
    for j in range(heads_each):
        each(1, lambda offset: o_copy(j, offset).wait_send())

    for j in range(heads_each):
        each(1, lambda offset: o_copy(j, offset).wait_recv())


def exchange(
    query_rows, key_rows, value_rows, query_tangent, key_tangent, value_tangent, query_gain, key_gain
):
    n_head, n_blk = lax.axis_size("head"), lax.axis_size("blk")
    rows, width = query_rows.shape[1:]
    ring = n_blk // 4
    chips = n_head * ring
    heads = width // HD
    heads_each = heads // chips
    first = lax.axis_index("blk") * rows * n_head + lax.axis_index("head") * rows
    cosine, sine = rotation(first, rows, HD)
    even = (jnp.arange(HD) % 2 == 0)[None, :]
    tables = (cosine, jnp.where(even, -sine, 0.0), jnp.where(even, 0.0, sine))
    arrays = [a[0] for a in (query_rows, key_rows, value_rows, query_tangent, key_tangent, value_tangent)]
    kv, q = prepare(arrays, (query_gain[None], key_gain[None]), tables, heads_each)
    dma = pltpu.SemaphoreType.DMA
    queries = chips * rows
    vmem = pl.BlockSpec(memory_space=pltpu.VMEM)
    out = pl.pallas_call(
        functools.partial(joint_kernel, n_head, ring, heads_each, rows),
        out_shape=jax.ShapeDtypeStruct((heads, 2, rows, HD), jnp.bfloat16),
        in_specs=[vmem, vmem],
        out_specs=vmem,
        scratch_shapes=[
            pltpu.VMEM((2, heads_each, ARRAYS, 2 * queries, HD), jnp.bfloat16),
            pltpu.VMEM((heads_each, 2, queries, HD), jnp.bfloat16),
            pltpu.VMEM((heads_each, 2, queries, HD), jnp.bfloat16),
            pltpu.VMEM((queries, HD), jnp.float32),
            pltpu.VMEM((queries, HD), jnp.float32),
            pltpu.VMEM((queries, HD), jnp.float32),
            pltpu.VMEM((queries, HD), jnp.float32),
            pltpu.VMEM((queries, HD), jnp.float32),
            dma((2, heads_each, chips)),
            dma((2, heads_each, chips)),
            dma((2, heads_each, chips)),
            dma((2, heads_each, chips)),
            dma((chips,)),
            dma((chips,)),
            dma((heads_each, chips)),
            dma((heads_each, chips)),
        ],
        compiler_params=pltpu.CompilerParams(
            collective_id=0, has_side_effects=True, vmem_limit_bytes=60 * 1024 * 1024
        ),
    )(kv, q)
    flat = out.transpose(1, 2, 0, 3).reshape(2, 1, rows, width)
    return flat[0], flat[1]


def chosen(mesh):
    n_head, n_blk = mesh.shape["head"], mesh.shape["blk"]

    def run(*arrays):
        heads = arrays[0].shape[2] // HD
        rows = arrays[0].shape[1]
        if n_blk == GROUP and heads % (n_head * n_blk // 4) == 0 and rows % 8 == 0:
            return exchange(*arrays)
        return local(*arrays)

    return run


def solution(mesh):
    in_specs = (
        P("blk", "head", None),
        P("blk", "head", None),
        P("blk", "head", None),
        P("blk", "head", None),
        P("blk", "head", None),
        P("blk", "head", None),
        P(),
        P(),
    )
    out_specs = (P("blk", "head", None), P("blk", "head", None))
    return jax.shard_map(chosen(mesh), mesh=mesh, in_specs=in_specs, out_specs=out_specs, check_vma=False)
```
